256 devices in a mesh: pipe: 8 (over x, core), dp: 8 (over z), tensor: 4 (over y).
Axes of the slice: x: 4, y: 4, z: 8, core: 2. Of those that a mesh axis runs over, the one named last changes fastest.
Arguments:
- acts_in: bfloat16 [2, 1024, 4096], P(None, 'dp', 'tensor'), may hold values from -6 to 6
- weights: bfloat16 [8, 4096, 4096], P('pipe', None, 'tensor'), may hold values from -0.046875 to 0.046875
- cotangent: bfloat16 [2, 1024, 4096], P(None, 'dp', 'tensor'), may hold values from -6 to 6
- hist_act: float32 [8, 16], P('pipe'), may hold values from 2 to 12
- hist_weight: float32 [8, 16], P('pipe'), may hold values from 0.01 to 0.1
- hist_grad: float32 [8, 16], P('pipe'), may hold values from 2 to 12
Outputs:
- section_acts: bfloat16 [8, 2, 1024, 4096], P('pipe', None, 'dp', 'tensor')
- section_grads: bfloat16 [8, 2, 1024, 4096], P('pipe', None, 'dp', 'tensor')
- weight_grad: bfloat16 [8, 4096, 4096], P('pipe', 'dp', 'tensor')
- new_hist_act: float32 [8, 16], P('pipe')
- new_hist_weight: float32 [8, 16], P('pipe')
- new_hist_grad: float32 [8, 16], P('pipe')
The draws below stay inside these ranges and needn't reach their ends.
All inputs are finite; a program needn't handle non-finite values.
Results may differ from the reference program's by a relative error of at most 0.025.
Values may be sent and summed in bfloat16 or wider, within the bound.
A program may use at most 128 MiB of HBM per device.

```python
import math
import jax
import jax.numpy as jnp
from jax import lax

D = 4096
ROWS = 128
MICRO = 2
HIST = 16
SECTIONS = 8
BATCH = 1024
N_DP = 8
N_TENSOR = 4


def steps_of(key, dims, split, least, high):
    factor_of, own = 1.0, jax.random.fold_in(key, 6)
    for axis_at, blocks in split:
        draws = jnp.exp(jax.random.uniform(jax.random.fold_in(own, axis_at), (blocks,), jnp.float32, least / len(split), high / len(split)))
        factor_of = factor_of * jnp.repeat(draws, dims[axis_at] // blocks).reshape([-1 if axis == axis_at else 1 for axis in range(len(dims))])
    return factor_of


def centred(rng, shape, scale, reach, pieces=(), kind=jnp.bfloat16):
    factor_of = steps_of(rng, shape, pieces, -0.22, 0.18) if pieces else 1.0
    result = jax.random.normal(rng, shape, jnp.float32) * scale * factor_of
    return jnp.minimum(jnp.maximum(result, -reach), reach).astype(kind)


def setup_inputs(seed: int = 0) -> dict:
    seeds = jax.random.split(jax.random.key(seed), 7)
    acts_in = centred(seeds[0], (MICRO, BATCH, D), 1.0, 6.0, ((1, 8), (2, 4)))
    weights = centred(seeds[1], (SECTIONS, D, D), (4 * D) ** -0.5, 0.046875, ((0, 8), (2, 4)))
    cotangent = centred(seeds[2], (MICRO, BATCH, D), 1.0, 6.0, ((1, 8), (2, 4)))
    hist_act = jnp.clip(jnp.exp(math.log(12.0) - 1.7917595 * jax.random.uniform(seeds[3], (SECTIONS, HIST), jnp.float32) ** steps_of(seeds[3], (SECTIONS, HIST), ((0, 8),), -0.2, 0.2)), 2.0, 12.0)
    hist_weight = jnp.clip(jnp.exp(math.log(0.1) - 2.3025851 * jax.random.uniform(seeds[4], (SECTIONS, HIST), jnp.float32) ** steps_of(seeds[4], (SECTIONS, HIST), ((0, 8),), -0.2, 0.2)), 0.01, 0.1)
    hist_grad = jnp.clip(jnp.exp(math.log(12.0) - 1.7917595 * jax.random.uniform(seeds[5], (SECTIONS, HIST), jnp.float32) ** steps_of(seeds[5], (SECTIONS, HIST), ((0, 8),), -0.2, 0.2)), 2.0, 12.0)
    return {"acts_in": acts_in, "weights": weights, "cotangent": cotangent, "hist_act": hist_act, "hist_weight": hist_weight, "hist_grad": hist_grad}


def quantize(values, factor, limit_value):
    return jnp.clip(values.astype(jnp.float32) * factor, -limit_value, limit_value).astype(jnp.bfloat16)


def settle(values):
    return lax.optimization_barrier(values.astype(jnp.bfloat16)).astype(jnp.float32)


def roll_history(history, newest):
    return jnp.concatenate([newest[:, None], history[:, :-1]], axis=1)


def reference(acts_in, weights, cotangent, hist_act, hist_weight, hist_grad):
    section_count = weights.shape[0]
    full_width = weights.shape[1]
    block_width = full_width // N_TENSOR
    current = acts_in.reshape(-1, full_width)
    act_factors = []
    weight_factors = []
    quant_acts = []
    quant_weights = []
    outputs = []
    act_peaks = []
    weight_peaks = []
    for section_index in range(section_count):
        act_factor = 448.0 / jnp.max(hist_act[section_index])
        weight_factor = 448.0 / jnp.max(hist_weight[section_index])
        quant_weight = quantize(weights[section_index], weight_factor, 448.0)
        quant_act = quantize(current, act_factor, 448.0)
        act_peaks.append(jnp.max(jnp.abs(current.astype(jnp.float32))))
        weight_peaks.append(jnp.max(jnp.abs(weights[section_index].astype(jnp.float32))))
        mixed_terms = jnp.dot(quant_act, quant_weight, preferred_element_type=jnp.float32) * (1.0 / (act_factor * weight_factor))
        current = (current.astype(jnp.float32) + mixed_terms).astype(jnp.bfloat16)
        outputs.append(current.reshape(MICRO, -1, full_width))
        act_factors.append(act_factor)
        weight_factors.append(weight_factor)
        quant_acts.append(quant_act)
        quant_weights.append(quant_weight)
    gradient = (cotangent.reshape(-1, full_width).astype(jnp.float32) * current.astype(jnp.float32)).astype(jnp.bfloat16)
    grads_out = [None] * section_count
    weight_sums = [None] * section_count
    grad_peaks = [None] * section_count
    for section_index in reversed(range(section_count)):
        grad_factor = 57344.0 / jnp.max(hist_grad[section_index])
        grad_peaks[section_index] = jnp.max(jnp.abs(gradient.astype(jnp.float32)))
        quant_grad = quantize(gradient, grad_factor, 57344.0)
        backward_factor = 1.0 / (grad_factor * weight_factors[section_index])
        sum_total = jnp.zeros((gradient.shape[0], full_width), jnp.float32)
        for shard_part in range(N_TENSOR):
            column_span = slice(shard_part * block_width, (shard_part + 1) * block_width)
            product_term = jnp.dot(quant_grad[:, column_span], quant_weights[section_index][:, column_span].T, preferred_element_type=jnp.float32) * backward_factor
            sum_total = sum_total + settle(product_term)
        gradient = (gradient.astype(jnp.float32) + sum_total).astype(jnp.bfloat16)
        grads_out[section_index] = gradient.reshape(MICRO, -1, full_width)
        update_factor = 1.0 / (act_factors[section_index] * grad_factor)
        acts_split = quant_acts[section_index].reshape(MICRO, N_DP, ROWS, full_width)
        grads_split = quant_grad.reshape(MICRO, N_DP, ROWS, full_width)
        weight_sum = jnp.zeros((full_width, full_width), jnp.float32)
        for dp_rank in range(N_DP):
            left_rows = acts_split[:, dp_rank].reshape(-1, full_width)
            right_rows = grads_split[:, dp_rank].reshape(-1, full_width)
            weight_sum = weight_sum + settle(jnp.dot(left_rows.T, right_rows, preferred_element_type=jnp.float32) * update_factor)
        weight_sums[section_index] = weight_sum.astype(jnp.bfloat16)
    section_acts = jnp.stack(outputs)
    section_grads = jnp.stack(grads_out)
    weight_grad = jnp.stack(weight_sums)
    new_hist_act = roll_history(hist_act, jnp.stack(act_peaks))
    new_hist_weight = roll_history(hist_weight, jnp.stack(weight_peaks))
    new_hist_grad = roll_history(hist_grad, jnp.stack(grad_peaks))
    return (section_acts, section_grads, weight_grad, new_hist_act, new_hist_weight, new_hist_grad)
```

```python
import functools

import jax
import jax.numpy as jnp
from jax import lax
from jax.experimental import pallas as pl
from jax.experimental.pallas import tpu as pltpu
from jax.sharding import PartitionSpec as P

MESH = pl.DeviceIdType.MESH
PIECES = 4


def kernel(S, N, T, NC, RC, F, FA,
           acts, weights, cot, hist_a, hist_w, hist_g,
           out_acts, out_grads, out_w, out_top,
           w, x, xq, xo, acc, pt, pr, fr, gin, gout, G, A, dw, dwb, pz, py, amax, gmax,
           w_sem, i_ss, x_ss, x_rs, A_ss, A_rs, p_ss, p_rs, f_rs,
           G_ss, G_rs, b_ss, b_rs, z_ss, z_rs, y_ss, y_rs, o_sem, ow_sem):
    s, d, t = lax.axis_index("pipe"), lax.axis_index("dp"), lax.axis_index("tensor")
    last = S - 1
    bf, f32 = jnp.bfloat16, jnp.float32
    late = s >= last - 1
    up = jnp.minimum(s + 1, last)
    down = jnp.maximum(s - 1, 0)
    ratio = N // T
    far_hops = N // 2
    near_hops = N - 1 - far_hops
    offsets = [T // 2] + [o for o in range(1, T) if o != T // 2]

    def remote(src, dst, ss, rsem, **where):
        return pltpu.make_async_remote_copy(
            src_ref=src, dst_ref=dst, send_sem=ss, recv_sem=rsem,
            device_id=where, device_id_type=MESH)

    def peer(o):
        return lax.rem(t + o, T)

    def row(k):
        return lax.rem(d + k, N)

    loads = [pltpu.make_async_copy(weights.at[b], w.at[b], w_sem.at[b]) for b in range(T)]
    for copy in loads:
        copy.start()

    barrier = pltpu.get_barrier_semaphore()
    for k in range(1, N):
        pl.semaphore_signal(barrier, inc=1, device_id={"dp": row(k)}, device_id_type=MESH)
    for o in range(1, T):
        pl.semaphore_signal(barrier, inc=1, device_id={"tensor": peer(o)}, device_id_type=MESH)

    @pl.when(s > 0)
    def _():
        for j in range(T):
            pl.semaphore_signal(barrier, inc=1, device_id={"pipe": s - 1, "tensor": j}, device_id_type=MESH)

    @pl.when(s < last)
    def _():
        for j in range(T):
            pl.semaphore_signal(barrier, inc=1, device_id={"pipe": s + 1, "tensor": j}, device_id_type=MESH)

    lim_a = jnp.max(hist_a[...], axis=1, keepdims=True).astype(bf)
    lim_w = jnp.max(hist_w[...], axis=1, keepdims=True).astype(bf)
    lim_g = jnp.max(hist_g[...], axis=1, keepdims=True).astype(bf)

    def clip(v, lim):
        return jnp.minimum(jnp.maximum(v, -lim), lim)

    def fold(v):
        return jnp.max(jnp.abs(v).reshape(-1, 16, v.shape[-1]), axis=0)

    amax[...] = jnp.zeros_like(amax)
    gmax[...] = jnp.zeros_like(gmax)

    near = (s > 0).astype(jnp.int32) + (s < last).astype(jnp.int32)
    pl.semaphore_wait(barrier, N - 1 + T - 1 + T * near)

    def first_copy(c, o):
        return remote(acts.at[c], x.at[c, t], i_ss.at[c, o], x_rs.at[c, t], tensor=peer(o))

    def x_copy(c, j):
        return remote(xo.at[c], x.at[c, t], x_ss.at[c, j], x_rs.at[c, t], pipe=up, tensor=j)

    def x_arrival(c, j):
        return remote(xo.at[c], x.at[c, j], x_ss.at[c, j], x_rs.at[c, j], pipe=down, tensor=j)

    def block_of(e):
        start = lax.rem(e, ratio) * FA
        return lax.div(e, ratio), pl.ds(pl.multiple_of(start, FA), FA)

    def A_copy(c, k):
        e = row(k)
        b, cols = block_of(e)
        return remote(xq.at[c, b, :, cols], A.at[c, d], A_ss.at[c, k], A_rs.at[c, k], dp=e)

    def A_arrival(c, k):
        r = row(N - k)
        return remote(A.at[c, r], A.at[c, r], A_ss.at[c, k], A_rs.at[c, k], dp=r)

    def p_copy(c, j):
        return remote(pt.at[c, j], pr.at[c, t], p_ss.at[c, j], p_rs.at[c, t], pipe=down, tensor=j)

    def p_arrival(c, j):
        return remote(pt.at[c, j], pr.at[c, j], p_ss.at[c, j], p_rs.at[c, j], pipe=up, tensor=j)

    def f_copy(c, o):
        j = peer(o)
        return remote(pt.at[c, j], fr.at[c, t], p_ss.at[c, j], f_rs.at[c, t], tensor=j)

    def f_arrival(c, o):
        j = peer(o)
        return remote(pt.at[c, j], fr.at[c, j], p_ss.at[c, j], f_rs.at[c, j], tensor=j)

    def back_copy(c):
        return remote(gin.at[c], out_grads.at[c], b_ss.at[c], b_rs.at[c], pipe=up)

    def back_arrival(c):
        return remote(gin.at[c], out_grads.at[c], b_ss.at[c], b_rs.at[c], pipe=down)

    def turn(c):
        return jnp.where(lax.rem(c, 2) == 0, 1, N - 1)

    def G_copy(c, way, h):
        ahead = turn(c) if way == 0 else N - turn(c)
        r = row((h - 1) * (N - ahead))
        return remote(G.at[c, r], G.at[c, r], G_ss.at[c, way, h - 1], G_rs.at[c, way, h - 1],
                      dp=row(ahead))

    def G_arrival(c, way, h):
        ahead = turn(c) if way == 0 else N - turn(c)
        r = row(h * (N - ahead))
        return remote(G.at[c, r], G.at[c, r], G_ss.at[c, way, h - 1], G_rs.at[c, way, h - 1],
                      dp=row(ahead))

    def z_copy(k):
        return remote(pz.at[0], pz.at[k], z_ss.at[k], z_rs.at[k], dp=row(k))

    def y_copy(o):
        return remote(py.at[0], py.at[o], y_ss.at[o], y_rs.at[o], tensor=peer(o))

    def acts_out(c):
        return pltpu.make_async_copy(xo.at[c], out_acts.at[c], o_sem.at[0, c])

    def grads_out(c):
        return pltpu.make_async_copy(gout.at[c], out_grads.at[c], o_sem.at[1, c])

    def each_chunk(body):
        def step(c, _):
            body(c)
            return 0

        lax.fori_loop(0, NC, step, 0)

    @pl.when(s == 0)
    def _():
        def body(c):
            x[c, t] = acts[c]
            for o in offsets:
                first_copy(c, o).start()

        each_chunk(body)

    dw[...] = jnp.zeros_like(dw)

    peak = jnp.zeros((16, F), bf)
    for b in range(T):
        loads[b].wait()

        def squeeze(i, m, b=b):
            rows = pl.ds(pl.multiple_of(i * 128, 128), 128)
            v = w[b, rows]
            w[b, rows] = clip(v, lim_w)
            return jnp.maximum(m, fold(v))

        peak = lax.fori_loop(0, F // 128, squeeze, peak)
    top_w = jnp.max(peak.astype(f32), keepdims=True).reshape(1, 1)
    pz[0] = jnp.broadcast_to(top_w, (8, 128))

    crossing = jnp.logical_and(s > 0, lax.rem(s, 2) == 0)
    middle = [o for o in range(1, T) if o != T // 2]

    def forward(c):
        order = [jnp.where(crossing, T // 2, 0)] + middle + [jnp.where(crossing, 0, T // 2)]
        for k, o in enumerate(order):
            j = peer(o)

            @pl.when(jnp.logical_or(s > 0, j != t))
            def _():
                x_arrival(c, j).wait_recv()

            q = clip(x[c, j], lim_a)
            xq[c, j] = q
            y = jnp.dot(q, w[j], preferred_element_type=f32)
            if k == 0:
                acc[...] = y
            elif k < T - 1:
                acc[...] += y
            else:
                xo[c] = (acc[...] + y + x[c, t].astype(f32)).astype(bf)

        @pl.when(s < last)
        def _():
            for o in offsets + [0]:
                x_copy(c, peer(o)).start()

        acts_out(c).start()
        b, cols = block_of(d)
        A[c, d] = xq[c, b, :, cols]
        amax[...] = jnp.maximum(amax[...], fold(x[c, t]))

        @pl.when(jnp.logical_not(late))
        def _():
            send_A(c)

    def send_A(c):
        for k in range(1, N):
            A_copy(c, k).start()

    def backward(c):
        @pl.when(s == last)
        def _():
            gin[c] = (cot[c].astype(f32) * xo[c].astype(f32)).astype(bf)

        @pl.when(s < last)
        def _():
            for o in range(T):
                p_arrival(c, peer(o)).wait_recv()
            total = pr[c, 0].astype(f32)
            for j in range(1, T):
                total = total + pr[c, j].astype(f32)
            gin[c] = total.astype(bf)
            back_copy(c).start()

        g = gin[c]
        q = clip(g, lim_g)
        G[c, d] = q
        for way in range(2):
            G_copy(c, way, 1).start()
        for o in offsets + [0]:
            b = peer(o)
            y = lax.dot_general(q, w[b], (((1,), (1,)), ((), ())), preferred_element_type=f32)
            if o == 0:
                y = y + g.astype(f32)
            pt[c, b] = y.astype(bf)

            @pl.when(s > 0)
            def _():
                p_copy(c, b).start()

            if o:
                @pl.when(s == 0)
                def _():
                    f_copy(c, o).start()

        gmax[...] = jnp.maximum(gmax[...], fold(g))

        @pl.when(c == NC - 1)
        def _():
            line = lax.broadcasted_iota(jnp.int32, (8, 128), 0)
            top_a = jnp.max(amax[...].astype(f32), keepdims=True).reshape(1, 1)
            top_g = jnp.max(gmax[...].astype(f32), keepdims=True).reshape(1, 1)
            pz[0] = jnp.where(line == 0, top_a, jnp.where(line == 1, pz[0], top_g))
            for k in range(1, N):
                z_copy(k).start()

    def finish_grads(c):
        total = pt[c, t].astype(f32)
        for o in range(1, T):
            f_arrival(c, o).wait_recv()
            total = total + fr[c, peer(o)].astype(f32)
        gout[c] = total.astype(bf)
        grads_out(c).start()

    def relay(c, h):
        @pl.when(jnp.logical_and(c >= 0, c < NC))
        def _():
            for way, hops in ((0, far_hops), (1, near_hops)):
                if h <= hops:
                    G_arrival(c, way, h).wait_recv()
                if h < hops:
                    G_copy(c, way, h + 1).start()

    def update(c):
        for k in range(1, N):
            A_arrival(c, k).wait_recv()
        tile = 256

        def body(n, _):
            cols = pl.ds(pl.multiple_of(n * tile, tile), tile)
            y = lax.dot_general(A[c, :, :, cols].reshape(N * RC, tile), G[c].reshape(N * RC, F),
                                (((0,), (0,)), ((), ())), preferred_element_type=f32)
            y = dw[cols, :] + y
            dw[cols, :] = y
            dwb[cols, :] = y.astype(bf)
            return 0

        lax.fori_loop(0, FA // tile, body, 0)

    def after(c):
        @pl.when(jnp.logical_and(late, c < NC))
        def _():
            send_A(c)

        for h in range(1, far_hops + 1):
            relay(c - h, h)

        @pl.when(jnp.logical_and(s == 0, jnp.logical_and(c >= 1, c <= NC)))
        def _():
            finish_grads(c - 1)

        @pl.when(c == NC + 2)
        def _():
            for k in range(1, N):
                z_copy(k).wait_recv()
            py[0] = jnp.max(pz[...], axis=0)
            for o in range(1, T):
                y_copy(o).start()

        @pl.when(c >= far_hops)
        def _():
            update(c - far_hops)

    def slot(i, _):
        m = i - NC
        is_last = s == last
        even = lax.rem(i, 2) == 0
        half = lax.div(i, 2)
        later = i >= 2 * NC
        paired = m < 2 * NC
        is_fwd = jnp.where(is_last, jnp.logical_and(even, i < 2 * NC), i < NC)
        c_fwd = jnp.where(is_last, half, i)
        early_bwd = jnp.logical_and(jnp.logical_and(m >= 0, paired), lax.rem(m + NC, 2) == NC % 2)
        is_bwd = jnp.where(is_last, jnp.logical_and(jnp.logical_not(even), i < 2 * NC),
                           jnp.where(late, jnp.logical_and(m >= 0, m < NC), early_bwd))
        c_bwd = jnp.where(is_last, half, jnp.where(late, m, lax.div(m, 2)))
        is_after = jnp.logical_and(jnp.logical_not(is_fwd), jnp.logical_not(is_bwd))
        c_after = jnp.where(late, i - 2 * NC, jnp.where(paired, lax.div(m, 2), m - NC))

        @pl.when(is_fwd)
        def _():
            forward(c_fwd)

        @pl.when(is_bwd)
        def _():
            backward(c_bwd)

        @pl.when(is_after)
        def _():
            after(c_after)

        return 0

    lax.fori_loop(0, 3 * NC + far_hops, slot, 0)

    out = pltpu.make_async_copy(dwb, out_w, ow_sem)
    out.start()

    for o in range(1, T):
        y_copy(o).wait_recv()
    out_top[...] = jnp.max(py[...], axis=0)

    def drain(c):
        for k in range(1, N):
            A_copy(c, k).wait_send()
        for way, hops in ((0, far_hops), (1, near_hops)):
            for h in range(1, hops + 1):
                G_copy(c, way, h).wait_send()
        acts_out(c).wait()

        @pl.when(s == 0)
        def _():
            for o in range(1, T):
                first_copy(c, o).wait_send()
                f_copy(c, o).wait_send()
            grads_out(c).wait()

        @pl.when(s > 0)
        def _():
            for j in range(T):
                p_copy(c, j).wait_send()
            back_arrival(c).wait_recv()

        @pl.when(s < last)
        def _():
            for j in range(T):
                x_copy(c, j).wait_send()
            back_copy(c).wait_send()

    each_chunk(drain)
    for k in range(1, N):
        z_copy(k).wait_send()
    for o in range(1, T):
        y_copy(o).wait_send()
    out.wait()


def finish(acts, grads, dw, top, hist_a, hist_w, hist_g,
           out_acts, out_grads, out_w, out_ha, out_hw, out_hg, held_a, held_g, held_w, in_sem, out_sem):
    half = dw.shape[0] // 2
    moves = [(acts, held_a, out_acts.at[0]), (grads, held_g, out_grads.at[0])]
    for i in range(2):
        rows = pl.ds(i * half, half)
        moves.append((dw.at[rows], held_w.at[rows], out_w.at[0, rows]))
    inward = [pltpu.make_async_copy(src, held, in_sem.at[0, i]) for i, (src, held, _) in enumerate(moves)]
    outward = [pltpu.make_async_copy(held, dst, out_sem.at[0, i]) for i, (_, held, dst) in enumerate(moves)]
    for copy in inward:
        copy.start()
    peaks = top[...]
    for row, (hist, out_hist) in enumerate(((hist_a, out_ha), (hist_w, out_hw), (hist_g, out_hg))):
        old = hist[...]
        out_hist[...] = jnp.concatenate([peaks[row:row + 1, 0:1], old[:, :-1]], axis=1)
    for copy, onward in zip(inward, outward):
        copy.wait()
        onward.start()
    for onward in outward:
        onward.wait()


def shards(acts_in, weights, cotangent, hist_act, hist_weight, hist_grad):
    S, N, T = lax.axis_size("pipe"), lax.axis_size("dp"), lax.axis_size("tensor")
    M, R, F = acts_in.shape
    NC, RC = M * PIECES, R // PIECES
    FA = T * F // N
    bf, f32 = jnp.bfloat16, jnp.float32
    dma = pltpu.SemaphoreType.DMA
    vmem = pl.BlockSpec(memory_space=pltpu.VMEM)
    anyw = pl.BlockSpec(memory_space=pl.ANY)
    hist = jax.ShapeDtypeStruct(hist_act.shape, f32)
    chunk = (NC, RC, F)
    acts, grads, dw, top = pl.pallas_call(
        functools.partial(kernel, S, N, T, NC, RC, F, FA),
        out_shape=(jax.ShapeDtypeStruct(chunk, bf), jax.ShapeDtypeStruct(chunk, bf),
                   jax.ShapeDtypeStruct((FA, F), bf), jax.ShapeDtypeStruct((8, 128), f32)),
        in_specs=[vmem, anyw, vmem, vmem, vmem, vmem],
        out_specs=(anyw, anyw, anyw, vmem),
        scratch_shapes=[
            pltpu.VMEM((T, F, F), bf),
            pltpu.VMEM((NC, T, RC, F), bf),
            pltpu.VMEM((NC, T, RC, F), bf),
            pltpu.VMEM(chunk, bf),
            pltpu.VMEM((RC, F), f32),
            pltpu.VMEM((NC, T, RC, F), bf),
            pltpu.VMEM((NC, T, RC, F), bf),
            pltpu.VMEM((NC, T, RC, F), bf),
            pltpu.VMEM(chunk, bf),
            pltpu.VMEM(chunk, bf),
            pltpu.VMEM((NC, N, RC, F), bf),
            pltpu.VMEM((NC, N, RC, FA), bf),
            pltpu.VMEM((FA, F), f32),
            pltpu.VMEM((FA, F), bf),
            pltpu.VMEM((N, 8, 128), f32),
            pltpu.VMEM((T, 8, 128), f32),
            pltpu.VMEM((16, F), bf),
            pltpu.VMEM((16, F), bf),
            dma((T,)), dma((NC, T)), dma((NC, T)), dma((NC, T)), dma((NC, N)), dma((NC, N)),
            dma((NC, T)), dma((NC, T)), dma((NC, T)),
            dma((NC, 2, N // 2)), dma((NC, 2, N // 2)), dma((NC,)), dma((NC,)),
            dma((N,)), dma((N,)), dma((T,)), dma((T,)), dma((2, NC)), dma(()),
        ],
        compiler_params=pltpu.CompilerParams(
            collective_id=0, has_side_effects=True, vmem_limit_bytes=60 * 2**20),
    )(acts_in.reshape(chunk), weights.reshape(T, F, F), cotangent.reshape(chunk),
      hist_act, hist_weight, hist_grad)
    full = (1, M, R, F)
    return pl.pallas_call(
        finish,
        out_shape=(jax.ShapeDtypeStruct(full, bf), jax.ShapeDtypeStruct(full, bf),
                   jax.ShapeDtypeStruct((1, FA, F), bf), hist, hist, hist),
        in_specs=[anyw, anyw, anyw, vmem, vmem, vmem, vmem],
        out_specs=(anyw, anyw, anyw, vmem, vmem, vmem),
        scratch_shapes=[pltpu.VMEM((M, R, F), bf), pltpu.VMEM((M, R, F), bf),
                        pltpu.VMEM((FA, F), bf), dma((2, 4)), dma((2, 4))],
        compiler_params=pltpu.CompilerParams(vmem_limit_bytes=60 * 2**20),
    )(acts.reshape(M, R, F), grads.reshape(M, R, F), dw, top, hist_act, hist_weight, hist_grad)


def solution(mesh):
    placed = (P(None, "dp", "tensor"), P("pipe", None, "tensor"), P(None, "dp", "tensor"),
              P("pipe", None), P("pipe", None), P("pipe", None))
    return jax.shard_map(
        shards, mesh=mesh, in_specs=placed,
        out_specs=(P("pipe", None, "dp", "tensor"), P("pipe", None, "dp", "tensor"),
                   P("pipe", "dp", "tensor"), P("pipe", None), P("pipe", None), P("pipe", None)),
        check_vma=False)
```

```python
import functools

import jax
import jax.numpy as jnp
from jax import lax
from jax.experimental import pallas as pl
from jax.experimental.pallas import tpu as pltpu
from jax.sharding import PartitionSpec as P

MESH = pl.DeviceIdType.MESH
PIECES = 4
AHEAD = 4
LAG = 2
GROUP = 4


def kernel(S, N, T, NC, RC, F, FA,
           acts, weights, cot, hist_a, hist_w, hist_g,
           out_acts, out_grads, out_w, out_top,
           w, wt, x, xq, xo, acc, pt, pr, gin, gout, G, A, dw, dwb, pz, py, amax, gmax,
           w_sem, i_ss, x_ss, x_rs, A_ss, A_rs, p_ss, p_rs,
           G_ss, G_rs, b_ss, b_rs, z_ss, z_rs, y_ss, y_rs, o_sem, ow_sem):
    s, d, t = lax.axis_index("pipe"), lax.axis_index("dp"), lax.axis_index("tensor")
    last = S - 1
    bf, f32 = jnp.bfloat16, jnp.float32
    late = s >= S // 2
    level = (s == 0).astype(jnp.int32)
    up = jnp.minimum(s + 1, last)
    down = jnp.maximum(s - 1, 0)
    ratio = N // T
    far_hops = N // 2
    near_hops = N - 1 - far_hops
    offsets = [T // 2] + [o for o in range(1, T) if o != T // 2]

    def remote(src, dst, ss, rsem, **where):
        return pltpu.make_async_remote_copy(
            src_ref=src, dst_ref=dst, send_sem=ss, recv_sem=rsem,
            device_id=where, device_id_type=MESH)

    def peer(o):
        return lax.rem(t + o, T)

    def row(k):
        return lax.rem(d + k, N)

    loads = [pltpu.make_async_copy(weights.at[b], w.at[b], w_sem.at[b]) for b in range(T)]
    for copy in loads:
        copy.start()

    barrier = pltpu.get_barrier_semaphore()
    for k in range(1, N):
        pl.semaphore_signal(barrier, inc=1, device_id={"dp": row(k)}, device_id_type=MESH)
    for o in range(1, T):
        pl.semaphore_signal(barrier, inc=1, device_id={"tensor": peer(o)}, device_id_type=MESH)

    @pl.when(s > 0)
    def _():
        for j in range(T):
            pl.semaphore_signal(barrier, inc=1, device_id={"pipe": s - 1, "tensor": j}, device_id_type=MESH)

    @pl.when(s < last)
    def _():
        for j in range(T):
            pl.semaphore_signal(barrier, inc=1, device_id={"pipe": s + 1, "tensor": j}, device_id_type=MESH)

    lim_a = jnp.max(hist_a[...], axis=1, keepdims=True).astype(bf)
    lim_w = jnp.max(hist_w[...], axis=1, keepdims=True).astype(bf)
    lim_g = jnp.max(hist_g[...], axis=1, keepdims=True).astype(bf)

    def clip(v, lim):
        return jnp.minimum(jnp.maximum(v, -lim), lim)

    def fold(v):
        return jnp.max(jnp.abs(v).reshape(-1, 16, v.shape[-1]), axis=0)

    amax[...] = jnp.zeros_like(amax)
    gmax[...] = jnp.zeros_like(gmax)

    near = (s > 0).astype(jnp.int32) + (s < last).astype(jnp.int32)
    pl.semaphore_wait(barrier, N - 1 + T - 1 + T * near)

    def first_copy(c, o):
        return remote(acts.at[c], x.at[c, t], i_ss.at[c, o], x_rs.at[c, t], tensor=peer(o))

    def x_copy(c, j):
        return remote(xo.at[c], x.at[c, t], x_ss.at[c, j], x_rs.at[c, t], pipe=up, tensor=j)

    def x_arrival(c, j):
        return remote(xo.at[c], x.at[c, j], x_ss.at[c, j], x_rs.at[c, j], pipe=down, tensor=j)

    def block_of(e):
        start = lax.rem(e, ratio) * FA
        return lax.div(e, ratio), pl.ds(pl.multiple_of(start, FA), FA)

    def A_copy(c, k):
        e = row(k)
        b, cols = block_of(e)
        return remote(xq.at[c, b, :, cols], A.at[c, d], A_ss.at[c, k], A_rs.at[c, k], dp=e)

    def A_arrival(c, k):
        r = row(N - k)
        return remote(A.at[c, r], A.at[c, r], A_ss.at[c, k], A_rs.at[c, k], dp=r)

    def p_copy(c, j):
        return remote(pt.at[c, j], pr.at[level, c, t], p_ss.at[c, j], p_rs.at[level, c, t],
                      pipe=down, tensor=j)

    def p_arrival(c, j):
        return remote(pt.at[c, j], pr.at[0, c, j], p_ss.at[c, j], p_rs.at[0, c, j], pipe=up, tensor=j)

    def f_arrival(c, j):
        return remote(pt.at[c, j], pr.at[1, c, j], p_ss.at[c, j], p_rs.at[1, c, j], tensor=j)

    def back_copy(c):
        return remote(gin.at[c], out_grads.at[c], b_ss.at[c], b_rs.at[c], pipe=up)

    def back_arrival(c):
        return remote(gin.at[c], out_grads.at[c], b_ss.at[c], b_rs.at[c], pipe=down)

    def turn(c):
        return jnp.where(lax.rem(c, 2) == 0, 1, N - 1)

    def G_copy(c, way, h):
        ahead = turn(c) if way == 0 else N - turn(c)
        r = row((h - 1) * (N - ahead))
        return remote(G.at[c, r], G.at[c, r], G_ss.at[c, way, h - 1], G_rs.at[c, way, h - 1],
                      dp=row(ahead))

    def G_arrival(c, way, h):
        ahead = turn(c) if way == 0 else N - turn(c)
        r = row(h * (N - ahead))
        return remote(G.at[c, r], G.at[c, r], G_ss.at[c, way, h - 1], G_rs.at[c, way, h - 1],
                      dp=row(ahead))

    def z_copy(k):
        return remote(pz.at[0], pz.at[k], z_ss.at[k], z_rs.at[k], dp=row(k))

    def y_copy(o):
        return remote(py.at[0], py.at[o], y_ss.at[o], y_rs.at[o], tensor=peer(o))

    def acts_out(c):
        return pltpu.make_async_copy(xo.at[c], out_acts.at[c], o_sem.at[0, c])

    def grads_out(c):
        return pltpu.make_async_copy(gout.at[c], out_grads.at[c], o_sem.at[1, c])

    def each_chunk(body):
        def step(c, _):
            body(c)
            return 0

        lax.fori_loop(0, NC, step, 0)

    def send_first(c):
        for o in offsets:
            first_copy(c, o).start()

    @pl.when(s == 0)
    def _():
        for c in range(AHEAD):
            send_first(c)

        def body(c):
            x[c, t] = acts[c]

        each_chunk(body)

    peak = jnp.zeros((16, F), bf)
    for b in range(T):
        loads[b].wait()

        def squeeze(i, m, b=b):
            rows = pl.ds(pl.multiple_of(i * 128, 128), 128)
            v = w[b, rows]
            w[b, rows] = clip(v, lim_w)
            return jnp.maximum(m, fold(v))

        peak = lax.fori_loop(0, F // 128, squeeze, peak)
    top_w = jnp.max(peak.astype(f32), keepdims=True).reshape(1, 1)
    pz[0] = jnp.broadcast_to(top_w, (8, 128))

    def flip_weights():
        def turn_block(i, _):
            b, n = lax.div(i, F // 128), lax.rem(i, F // 128)
            rows = pl.ds(pl.multiple_of(n * 128, 128), 128)
            wt[b, :, rows] = w[b, rows, :].T
            return 0

        lax.fori_loop(0, T * (F // 128), turn_block, 0)

    pl.when(late)(flip_weights)

    crossing = jnp.logical_and(s > 0, lax.rem(s, 2) == 0)
    middle = [o for o in range(1, T) if o != T // 2]

    def forward(c):
        first = peer(jnp.where(crossing, T // 2, 0))
        rest = [peer(o) for o in middle] + [peer(jnp.where(crossing, 0, T // 2))]

        @pl.when(s > 0)
        def _():
            x_arrival(c, first).wait_recv()

        q = clip(x[c, first], lim_a)
        xq[c, first] = q
        acc[...] = jnp.dot(q, w[first], preferred_element_type=f32)
        for j in rest:
            x_arrival(c, j).wait_recv()
        y = acc[...] + x[c, t].astype(f32)
        for j in rest:
            q = clip(x[c, j], lim_a)
            xq[c, j] = q
            y = y + jnp.dot(q, w[j], preferred_element_type=f32)
        xo[c] = y.astype(bf)

        @pl.when(s < last)
        def _():
            for o in offsets + [0]:
                x_copy(c, peer(o)).start()

        @pl.when(jnp.logical_and(s == 0, c + AHEAD < NC))
        def _():
            send_first(jnp.minimum(c + AHEAD, NC - 1))

        acts_out(c).start()
        send_A(c)
        b, cols = block_of(d)
        A[c, d] = xq[c, b, :, cols]
        amax[...] = jnp.maximum(amax[...], fold(x[c, t]))

    def send_A(c):
        for k in range(1, N):
            A_copy(c, k).start()

    def backward(c):
        @pl.when(s == last)
        def _():
            gin[c] = (cot[c].astype(f32) * xo[c].astype(f32)).astype(bf)

        @pl.when(s < last)
        def _():
            for o in range(T):
                p_arrival(c, peer(o)).wait_recv()
            total = pr[0, c, 0].astype(f32)
            for j in range(1, T):
                total = total + pr[0, c, j].astype(f32)
            gin[c] = total.astype(bf)
            back_copy(c).start()

        g = gin[c]
        q = clip(g, lim_g)
        G[c, d] = q
        for way in range(2):
            G_copy(c, way, 1).start()
        for o in offsets:
            b = peer(o)
            pt[c, b] = jnp.dot(q, wt[b], preferred_element_type=f32).astype(bf)
            p_copy(c, b).start()
        y = jnp.dot(q, wt[t], preferred_element_type=f32) + g.astype(f32)
        pt[c, t] = y.astype(bf)

        @pl.when(s > 0)
        def _():
            p_copy(c, t).start()

        gmax[...] = jnp.maximum(gmax[...], fold(g))

        @pl.when(c == NC - 1)
        def _():
            line = lax.broadcasted_iota(jnp.int32, (8, 128), 0)
            top_a = jnp.max(amax[...].astype(f32), keepdims=True).reshape(1, 1)
            top_g = jnp.max(gmax[...].astype(f32), keepdims=True).reshape(1, 1)
            pz[0] = jnp.where(line == 0, top_a, jnp.where(line == 1, pz[0], top_g))
            for k in range(1, N):
                z_copy(k).start()

    def finish_grads(c):
        total = pt[c, t].astype(f32)
        for o in range(1, T):
            f_arrival(c, peer(o)).wait_recv()
            total = total + pr[1, c, peer(o)].astype(f32)
        gout[c] = total.astype(bf)
        grads_out(c).start()

    def relay(c, h):
        @pl.when(jnp.logical_and(c >= 0, c < NC))
        def _():
            for way, hops in ((0, far_hops), (1, near_hops)):
                if h <= hops:
                    G_arrival(c, way, h).wait_recv()
                if h < hops:
                    G_copy(c, way, h + 1).start()

    def update(first):
        def arrived(c, _):
            for k in range(1, N):
                A_arrival(c, k).wait_recv()
            return 0

        lax.fori_loop(first, first + GROUP, arrived, 0)
        tile, depth = 256, GROUP * N * RC
        span = pl.ds(first, GROUP)

        def body(n, _):
            cols = pl.ds(pl.multiple_of(n * tile, tile), tile)
            y = lax.dot_general(A[span, :, :, cols].reshape(depth, tile), G[span].reshape(depth, F),
                                (((0,), (0,)), ((), ())), preferred_element_type=f32)
            if first:
                y = dw[cols, :] + y
            if first + GROUP < NC:
                dw[cols, :] = y
            else:
                dwb[cols, :] = y.astype(bf)
            return 0

        lax.fori_loop(0, FA // tile, body, 0)

    def after(c):
        for h in range(1, far_hops + 1):
            relay(c - LAG * h, h)

        @pl.when(jnp.logical_and(s == 0, jnp.logical_and(c >= 1, c <= NC)))
        def _():
            finish_grads(c - 1)

        @pl.when(c == NC + 2)
        def _():
            for k in range(1, N):
                z_copy(k).wait_recv()
            py[0] = jnp.max(pz[...], axis=0)
            for o in range(1, T):
                y_copy(o).start()

        for first in range(0, NC, GROUP):
            @pl.when(c == first + GROUP - 1 + LAG * far_hops)
            def _():
                update(first)

    def slot(i, _):
        m = i - NC
        is_last = s == last
        even = lax.rem(i, 2) == 0
        half = lax.div(i, 2)
        later = i >= 2 * NC
        paired = m < 2 * NC
        is_fwd = jnp.where(is_last, jnp.logical_and(even, i < 2 * NC), i < NC)
        c_fwd = jnp.where(is_last, half, i)
        early_bwd = jnp.logical_and(jnp.logical_and(m >= 0, paired), lax.rem(m + NC, 2) == NC % 2)
        is_bwd = jnp.where(is_last, jnp.logical_and(jnp.logical_not(even), i < 2 * NC),
                           jnp.where(late, jnp.logical_and(m >= 0, m < NC), early_bwd))
        c_bwd = jnp.where(is_last, half, jnp.where(late, m, lax.div(m, 2)))
        is_after = jnp.logical_and(jnp.logical_not(is_fwd), jnp.logical_not(is_bwd))
        c_after = jnp.where(late, i - 2 * NC, jnp.where(paired, lax.div(m, 2), m - NC))

        @pl.when(jnp.logical_and(i == NC, jnp.logical_not(late)))
        def _():
            flip_weights()

        @pl.when(is_fwd)
        def _():
            forward(c_fwd)

        @pl.when(is_bwd)
        def _():
            backward(c_bwd)

        @pl.when(is_after)
        def _():
            after(c_after)

        return 0

    lax.fori_loop(0, 3 * NC + LAG * far_hops, slot, 0)

    out = pltpu.make_async_copy(dwb, out_w, ow_sem)
    out.start()

    for o in range(1, T):
        y_copy(o).wait_recv()
    out_top[...] = jnp.max(py[...], axis=0)

    def drain(c):
        for k in range(1, N):
            A_copy(c, k).wait_send()
        for way, hops in ((0, far_hops), (1, near_hops)):
            for h in range(1, hops + 1):
                G_copy(c, way, h).wait_send()
        acts_out(c).wait()
        for o in range(1, T):
            p_copy(c, peer(o)).wait_send()

        @pl.when(s == 0)
        def _():
            for o in range(1, T):
                first_copy(c, o).wait_send()
            grads_out(c).wait()

        @pl.when(s > 0)
        def _():
            p_copy(c, t).wait_send()
            back_arrival(c).wait_recv()

        @pl.when(s < last)
        def _():
            for j in range(T):
                x_copy(c, j).wait_send()
            back_copy(c).wait_send()

    each_chunk(drain)
    for k in range(1, N):
        z_copy(k).wait_send()
    for o in range(1, T):
        y_copy(o).wait_send()
    out.wait()


def finish(acts, grads, dw, top, hist_a, hist_w, hist_g,
           out_acts, out_grads, out_w, out_ha, out_hw, out_hg, held_a, held_g, held_w, in_sem, out_sem):
    half = dw.shape[0] // 2
    moves = [(acts, held_a, out_acts.at[0]), (grads, held_g, out_grads.at[0])]
    for i in range(2):
        rows = pl.ds(i * half, half)
        moves.append((dw.at[rows], held_w.at[rows], out_w.at[0, rows]))
    inward = [pltpu.make_async_copy(src, held, in_sem.at[0, i]) for i, (src, held, _) in enumerate(moves)]
    outward = [pltpu.make_async_copy(held, dst, out_sem.at[0, i]) for i, (_, held, dst) in enumerate(moves)]
    for copy in inward:
        copy.start()
    peaks = top[...]
    for row, (hist, out_hist) in enumerate(((hist_a, out_ha), (hist_w, out_hw), (hist_g, out_hg))):
        old = hist[...]
        out_hist[...] = jnp.concatenate([peaks[row:row + 1, 0:1], old[:, :-1]], axis=1)
    for copy, onward in zip(inward, outward):
        copy.wait()
        onward.start()
    for onward in outward:
        onward.wait()


def shards(acts_in, weights, cotangent, hist_act, hist_weight, hist_grad):
    S, N, T = lax.axis_size("pipe"), lax.axis_size("dp"), lax.axis_size("tensor")
    M, R, F = acts_in.shape
    NC, RC = M * PIECES, R // PIECES
    FA = T * F // N
    bf, f32 = jnp.bfloat16, jnp.float32
    dma = pltpu.SemaphoreType.DMA
    vmem = pl.BlockSpec(memory_space=pltpu.VMEM)
    anyw = pl.BlockSpec(memory_space=pl.ANY)
    hist = jax.ShapeDtypeStruct(hist_act.shape, f32)
    chunk = (NC, RC, F)
    acts, grads, dw, top = pl.pallas_call(
        functools.partial(kernel, S, N, T, NC, RC, F, FA),
        out_shape=(jax.ShapeDtypeStruct(chunk, bf), jax.ShapeDtypeStruct(chunk, bf),
                   jax.ShapeDtypeStruct((FA, F), bf), jax.ShapeDtypeStruct((8, 128), f32)),
        in_specs=[vmem, anyw, vmem, vmem, vmem, vmem],
        out_specs=(anyw, anyw, anyw, vmem),
        scratch_shapes=[
            pltpu.VMEM((T, F, F), bf),
            pltpu.VMEM((T, F, F), bf),
            pltpu.VMEM((NC, T, RC, F), bf),
            pltpu.VMEM((NC, T, RC, F), bf),
            pltpu.VMEM(chunk, bf),
            pltpu.VMEM((RC, F), f32),
            pltpu.VMEM((NC, T, RC, F), bf),
            pltpu.VMEM((2, NC, T, RC, F), bf),
            pltpu.VMEM(chunk, bf),
            pltpu.VMEM(chunk, bf),
            pltpu.VMEM((NC, N, RC, F), bf),
            pltpu.VMEM((NC, N, RC, FA), bf),
            pltpu.VMEM((FA, F), f32),
            pltpu.VMEM((FA, F), bf),
            pltpu.VMEM((N, 8, 128), f32),
            pltpu.VMEM((T, 8, 128), f32),
            pltpu.VMEM((16, F), bf),
            pltpu.VMEM((16, F), bf),
            dma((T,)), dma((NC, T)), dma((NC, T)), dma((NC, T)), dma((NC, N)), dma((NC, N)),
            dma((NC, T)), dma((2, NC, T)),
            dma((NC, 2, N // 2)), dma((NC, 2, N // 2)), dma((NC,)), dma((NC,)),
            dma((N,)), dma((N,)), dma((T,)), dma((T,)), dma((2, NC)), dma(()),
        ],
        compiler_params=pltpu.CompilerParams(
            collective_id=0, has_side_effects=True, vmem_limit_bytes=60 * 2**20),
    )(acts_in.reshape(chunk), weights.reshape(T, F, F), cotangent.reshape(chunk),
      hist_act, hist_weight, hist_grad)
    full = (1, M, R, F)
    return pl.pallas_call(
        finish,
        out_shape=(jax.ShapeDtypeStruct(full, bf), jax.ShapeDtypeStruct(full, bf),
                   jax.ShapeDtypeStruct((1, FA, F), bf), hist, hist, hist),
        in_specs=[anyw, anyw, anyw, vmem, vmem, vmem, vmem],
        out_specs=(anyw, anyw, anyw, vmem, vmem, vmem),
        scratch_shapes=[pltpu.VMEM((M, R, F), bf), pltpu.VMEM((M, R, F), bf),
                        pltpu.VMEM((FA, F), bf), dma((2, 4)), dma((2, 4))],
        compiler_params=pltpu.CompilerParams(vmem_limit_bytes=60 * 2**20),
    )(acts.reshape(M, R, F), grads.reshape(M, R, F), dw, top, hist_act, hist_weight, hist_grad)


def solution(mesh):
    placed = (P(None, "dp", "tensor"), P("pipe", None, "tensor"), P(None, "dp", "tensor"),
              P("pipe", None), P("pipe", None), P("pipe", None))
    return jax.shard_map(
        shards, mesh=mesh, in_specs=placed,
        out_specs=(P("pipe", None, "dp", "tensor"), P("pipe", None, "dp", "tensor"),
                   P("pipe", "dp", "tensor"), P("pipe", None), P("pipe", None), P("pipe", None)),
        check_vma=False)
```

```python
import functools

import jax
import jax.numpy as jnp
from jax import lax
from jax.experimental import pallas as pl
from jax.experimental.pallas import tpu as pltpu
from jax.sharding import PartitionSpec as P

MESH = pl.DeviceIdType.MESH
PIECES = 8
AHEAD = 6
LAG = 2
WARM = 4
UPDATES = ((0, 8), (8, 4), (12, 4))
PAIR = 2
HALVES = 2


def kernel(S, N, T, NC, RC, F, FA,
           acts, weights, cot, hist_a, hist_w, hist_g,
           out_acts, out_grads, out_w, out_top,
           w, wt, x, xq, xo, acc, pt, pr, gin, gout, G, A, dw, dwb, pz, py, amax, gmax,
           w_sem, i_ss, x_ss, x_rs, A_ss, A_rs, B_ss, B_rs, p_ss, p_rs,
           G_ss, G_rs, b_ss, b_rs, z_ss, z_rs, y_ss, y_rs, o_sem, ow_sem):
    s, d, t = lax.axis_index("pipe"), lax.axis_index("dp"), lax.axis_index("tensor")
    last = S - 1
    bf, f32 = jnp.bfloat16, jnp.float32
    upper = s >= S // 2
    wide = s >= last - 1
    tail = LAG * (N // 2)
    level = (s == 0).astype(jnp.int32)
    up = jnp.minimum(s + 1, last)
    down = jnp.maximum(s - 1, 0)
    ratio = N // T
    far_hops = N // 2
    near_hops = N - 1 - far_hops
    offsets = [T // 2] + [o for o in range(1, T) if o != T // 2]

    def remote(src, dst, ss, rsem, **where):
        return pltpu.make_async_remote_copy(
            src_ref=src, dst_ref=dst, send_sem=ss, recv_sem=rsem,
            device_id=where, device_id_type=MESH)

    def peer(o):
        return lax.rem(t + o, T)

    def row(k):
        return lax.rem(d + k, N)

    loads = [pltpu.make_async_copy(weights.at[b], w.at[b], w_sem.at[b]) for b in range(T)]
    for copy in loads:
        copy.start()

    barrier = pltpu.get_barrier_semaphore()
    for k in range(1, N):
        pl.semaphore_signal(barrier, inc=1, device_id={"dp": row(k)}, device_id_type=MESH)
    for o in range(1, T):
        pl.semaphore_signal(barrier, inc=1, device_id={"tensor": peer(o)}, device_id_type=MESH)

    @pl.when(s > 0)
    def _():
        for j in range(T):
            pl.semaphore_signal(barrier, inc=1, device_id={"pipe": s - 1, "tensor": j}, device_id_type=MESH)

    @pl.when(s < last)
    def _():
        for j in range(T):
            pl.semaphore_signal(barrier, inc=1, device_id={"pipe": s + 1, "tensor": j}, device_id_type=MESH)

    lim_a = jnp.max(hist_a[...], axis=1, keepdims=True).astype(bf)
    lim_w = jnp.max(hist_w[...], axis=1, keepdims=True).astype(bf)
    lim_g = jnp.max(hist_g[...], axis=1, keepdims=True).astype(bf)

    def clip(v, lim):
        return jnp.minimum(jnp.maximum(v, -lim), lim)

    def fold(v):
        return jnp.max(jnp.abs(v).reshape(-1, 16, v.shape[-1]), axis=0)

    amax[...] = jnp.zeros_like(amax)
    gmax[...] = jnp.zeros_like(gmax)

    near = (s > 0).astype(jnp.int32) + (s < last).astype(jnp.int32)
    pl.semaphore_wait(barrier, N - 1 + T - 1 + T * near)

    def settled(ref, sem):
        return remote(ref, ref, sem, sem, tensor=peer(1))

    crossing = jnp.logical_and(s > 0, lax.rem(s, 2) == 0)
    crossing_up = lax.rem(s, 2) == 1

    def first_copy(c, o):
        return remote(acts.at[c], x.at[c, t], i_ss, x_rs.at[c, 1], tensor=peer(o))

    def x_copy(c, o, cols):
        lead = jnp.where(crossing_up, T // 2, 0) == o
        return remote(xo.at[c, :, cols], x.at[c, t, :, cols], x_ss,
                      x_rs.at[c, jnp.where(lead, 0, 1)], pipe=up, tensor=peer(o))

    def block_of(e):
        start = lax.rem(e, ratio) * FA
        return lax.div(e, ratio), pl.ds(pl.multiple_of(start, FA), FA)

    def A_copy(c, k):
        e = row(k)
        b, cols = block_of(e)
        return remote(xq.at[c, b, :, cols], A.at[c, d], A_ss, A_rs, dp=e)

    def B_copy(c, o):
        return remote(A.at[c], A.at[c], B_ss, B_rs, tensor=peer(o))

    def p_copy(c, j):
        return remote(pt.at[c, j], pr.at[level, c, t], p_ss, p_rs.at[level, c], pipe=down, tensor=j)

    def back_copy(c):
        return remote(gin.at[c], out_grads.at[c], b_ss, b_rs, pipe=up)

    def turn(c):
        return jnp.where(lax.rem(c, 2) == 0, 1, N - 1)

    def G_copy(c, way, h):
        ahead = turn(c) if way == 0 else N - turn(c)
        r = row((h - 1) * (N - ahead))
        return remote(G.at[c, r], G.at[c, r], G_ss, G_rs.at[c, h - 1], dp=row(ahead))

    def z_copy(k):
        return remote(pz.at[0], pz.at[k], z_ss, z_rs, dp=row(k))

    def y_copy(o):
        return remote(py.at[0], py.at[o], y_ss, y_rs, tensor=peer(o))

    def acts_out(c):
        return pltpu.make_async_copy(xo.at[c], out_acts.at[c], o_sem.at[0])

    def grads_out(c):
        return pltpu.make_async_copy(gout.at[c], out_grads.at[c], o_sem.at[1])

    def each_chunk(body):
        def step(c, _):
            body(c)
            return 0

        lax.fori_loop(0, NC, step, 0)

    def send_first(c):
        for o in offsets:
            first_copy(c, o).start()

    @pl.when(s == 0)
    def _():
        for c in range(AHEAD):
            send_first(c)

        def body(c):
            x[c, t] = acts[c]

        each_chunk(body)

    peak = jnp.zeros((16, F), bf)
    for b in range(T):
        loads[b].wait()

        def squeeze(i, m, b=b):
            rows = pl.ds(pl.multiple_of(i * 128, 128), 128)
            v = w[b, rows]
            w[b, rows] = clip(v, lim_w)
            return jnp.maximum(m, fold(v))

        peak = lax.fori_loop(0, F // 128, squeeze, peak)
    top_w = jnp.max(peak.astype(f32), keepdims=True).reshape(1, 1)
    pz[0] = jnp.broadcast_to(top_w, (8, 128))

    def flip_weights():
        def turn_block(i, _):
            b, n = lax.div(i, F // 128), lax.rem(i, F // 128)
            rows = pl.ds(pl.multiple_of(n * 128, 128), 128)
            wt[b, :, rows] = w[b, rows, :].T
            return 0

        lax.fori_loop(0, T * (F // 128), turn_block, 0)

    pl.when(upper)(flip_weights)

    middle = [o for o in range(1, T) if o != T // 2]

    def forward(c, n):
        first = peer(jnp.where(crossing, T // 2, 0))
        rest = [peer(o) for o in middle] + [peer(jnp.where(crossing, 0, T // 2))]
        span, high = pl.ds(c, n), n * RC

        @pl.when(s > 0)
        def _():
            for m in range(n):
                settled(x.at[c + m, 0], x_rs.at[c + m, 0]).wait_recv()

        q = clip(x[span, first], lim_a)
        xq[span, first] = q
        acc[pl.ds(0, high)] = jnp.dot(q.reshape(high, F), w[first], preferred_element_type=f32)
        for m in range(n):
            settled(x.at[c + m, pl.ds(0, T - 1)], x_rs.at[c + m, 1]).wait_recv()
        for j in rest:
            xq[span, j] = clip(x[span, j], lim_a)
        width = F // HALVES
        for k in range(HALVES):
            cols = pl.ds(k * width, width)
            y = acc[pl.ds(0, high), cols] + x[span, t, :, cols].reshape(high, width).astype(f32)
            for j in rest:
                y = y + jnp.dot(xq[span, j].reshape(high, F), w[j, :, cols], preferred_element_type=f32)
            xo[span, :, cols] = y.astype(bf).reshape(n, RC, width)

            @pl.when(s < last)
            def _():
                for m in range(n):
                    for o in offsets + [0]:
                        x_copy(c + m, o, cols).start()

        if n == 1:
            @pl.when(jnp.logical_and(s == 0, c + AHEAD < NC))
            def _():
                send_first(jnp.minimum(c + AHEAD, NC - 1))

        for m in range(n):
            acts_out(c + m).start()

            @pl.when(lax.rem(c + m, T) == t)
            def _():
                send_A(c + m)
                b, cols = block_of(d)
                A[c + m, d] = xq[c + m, b, :, cols]

        amax[...] = jnp.maximum(amax[...], fold(x[span, t]))

    def send_A(c):
        for k in range(1, N):
            A_copy(c, k).start()

    def backward(c, n):
        span, high = pl.ds(c, n), n * RC

        def last_grads():
            gin[span] = (cot[span].astype(f32) * xo[span].astype(f32)).astype(bf)

        def summed_grads():
            for m in range(n):
                settled(pr.at[0, c + m], p_rs.at[0, c + m]).wait_recv()
            total = pr[0, span, 0].astype(f32)
            for j in range(1, T):
                total = total + pr[0, span, j].astype(f32)
            gin[span] = total.astype(bf)
            for m in range(n):
                back_copy(c + m).start()

        if n == 1:
            summed_grads()
        else:
            pl.when(s == last)(last_grads)
            pl.when(s < last)(summed_grads)
        g = gin[span]
        q = clip(g, lim_g)
        G[span, d] = q
        for m in range(n):
            for way in range(2):
                G_copy(c + m, way, 1).start()
        q = q.reshape(high, F)
        for o in offsets:
            b = peer(o)
            pt[span, b] = jnp.dot(q, wt[b], preferred_element_type=f32).astype(bf).reshape(n, RC, F)
            for m in range(n):
                p_copy(c + m, b).start()
        y = jnp.dot(q, wt[t], preferred_element_type=f32) + g.reshape(high, F).astype(f32)
        pt[span, t] = y.astype(bf).reshape(n, RC, F)

        @pl.when(s > 0)
        def _():
            for m in range(n):
                p_copy(c + m, t).start()

        gmax[...] = jnp.maximum(gmax[...], fold(g))

        @pl.when(c == NC - n)
        def _():
            line = lax.broadcasted_iota(jnp.int32, (8, 128), 0)
            top_a = jnp.max(amax[...].astype(f32), keepdims=True).reshape(1, 1)
            top_g = jnp.max(gmax[...].astype(f32), keepdims=True).reshape(1, 1)
            pz[0] = jnp.where(line == 0, top_a, jnp.where(line == 1, pz[0], top_g))
            for k in range(1, N):
                z_copy(k).start()

    def finish_grads(c):
        settled(pr.at[1, c, pl.ds(0, T - 1)], p_rs.at[1, c]).wait_recv()
        total = pt[c, t].astype(f32)
        for o in range(1, T):
            total = total + pr[1, c, peer(o)].astype(f32)
        gout[c] = total.astype(bf)
        grads_out(c).start()

    def spread():
        settled(A.at[pl.ds(0, NC // T), pl.ds(0, N - 1)], A_rs).wait_recv()
        for m in range(NC // T):
            for o in offsets:
                B_copy(t + T * m, o).start()

    def relay(c, h):
        @pl.when(jnp.logical_and(c >= 0, c < NC))
        def _():
            ways = 2 if h <= near_hops else 1
            settled(G.at[c, pl.ds(0, ways)], G_rs.at[c, h - 1]).wait_recv()
            for way, hops in ((0, far_hops), (1, near_hops)):
                if h < hops:
                    G_copy(c, way, h + 1).start()

    def update(first, count):
        if first == 0:
            settled(A.at[pl.ds(0, NC - NC // T)], B_rs).wait_recv()
        tile, depth = 256, count * N * RC
        span = pl.ds(first, count)

        def body(n, _):
            cols = pl.ds(pl.multiple_of(n * tile, tile), tile)
            y = lax.dot_general(A[span, :, :, cols].reshape(depth, tile), G[span].reshape(depth, F),
                                (((0,), (0,)), ((), ())), preferred_element_type=f32)
            if first:
                y = dw[cols, :] + y
            if first + count < NC:
                dw[cols, :] = y
            else:
                dwb[cols, :] = y.astype(bf)
            return 0

        lax.fori_loop(0, FA // tile, body, 0)

    def after(c):
        for h in range(1, far_hops + 1):
            relay(c - LAG * h, h)

        @pl.when(jnp.logical_and(s == 0, jnp.logical_and(c >= 4, c < NC + 4)))
        def _():
            finish_grads(c - 4)

        @pl.when(jnp.logical_and(upper, c == jnp.where(wide, 4, NC)))
        def _():
            spread()

        @pl.when(c == NC + 1)
        def _():
            settled(pz.at[pl.ds(1, N - 1)], z_rs).wait_recv()
            py[0] = jnp.max(pz[...], axis=0)
            for o in range(1, T):
                y_copy(o).start()

        for first, count in UPDATES:
            @pl.when(c == max(NC, first + count - 1 + tail))
            def _():
                update(first, count)

    count = jnp.where(wide, NC // PAIR, NC)
    warm = jnp.where(s == last, 1, jnp.where(wide, WARM, count))

    def slot(i, _):
        m = i - count
        turned = i - warm
        mixed = jnp.logical_and(turned >= 0, i < 2 * count - warm)
        odd = lax.rem(i + 2 * NC - warm, 2) == 1
        ahead = jnp.logical_or(turned < 0, jnp.logical_and(mixed, odd))
        turn_c = jnp.where(turned < 0, i, jnp.where(mixed, lax.div(turned, 2) + jnp.where(odd, warm, 0), m))
        paired = m < 2 * NC
        even = lax.rem(i + NC, 2) == 0
        is_fwd = jnp.where(wide, jnp.logical_and(ahead, i < 2 * count), i < NC)
        is_bwd = jnp.where(wide, jnp.logical_and(jnp.logical_not(ahead), i < 2 * count),
                           jnp.logical_and(jnp.logical_and(m >= 0, paired), even))
        c_after = jnp.where(wide, i - 2 * count, jnp.where(paired, lax.div(m, 2), m - NC))
        is_after = jnp.logical_and(jnp.logical_not(jnp.logical_or(is_fwd, is_bwd)), c_after < NC + tail)
        c_fwd = jnp.where(wide, turn_c, i)
        c_bwd = jnp.where(wide, turn_c, lax.div(m, 2))

        @pl.when(jnp.logical_and(i == NC, jnp.logical_not(upper)))
        def _():
            flip_weights()
            spread()

        for body, on, c in ((forward, is_fwd, c_fwd), (backward, is_bwd, c_bwd)):
            @pl.when(jnp.logical_and(on, jnp.logical_not(wide)))
            def _():
                body(c, 1)

            @pl.when(jnp.logical_and(on, wide))
            def _():
                body(PAIR * c, PAIR)

        @pl.when(is_after)
        def _():
            after(c_after)

        return 0

    lax.fori_loop(0, 3 * NC + LAG * far_hops, slot, 0)

    out = pltpu.make_async_copy(dwb, out_w, ow_sem)
    out.start()

    settled(py.at[pl.ds(1, T - 1)], y_rs).wait_recv()
    out_top[...] = jnp.max(py[...], axis=0)

    settled(A.at[pl.ds(0, NC // T), pl.ds(0, N - 1)], A_ss).wait_send()
    settled(A.at[pl.ds(0, NC - NC // T)], B_ss).wait_send()
    settled(G.at[:, pl.ds(0, N - 1)], G_ss).wait_send()
    settled(pz.at[pl.ds(1, N - 1)], z_ss).wait_send()
    settled(py.at[pl.ds(1, T - 1)], y_ss).wait_send()
    pltpu.make_async_copy(xo, out_acts, o_sem.at[0]).wait()

    @pl.when(s == 0)
    def _():
        settled(x.at[:, pl.ds(0, T - 1)], i_ss).wait_send()
        settled(pt.at[:, pl.ds(0, T - 1)], p_ss).wait_send()
        pltpu.make_async_copy(gout, out_grads, o_sem.at[1]).wait()

    @pl.when(s > 0)
    def _():
        settled(pt, p_ss).wait_send()
        settled(out_grads, b_rs).wait_recv()

    @pl.when(s < last)
    def _():
        settled(x, x_ss).wait_send()
        settled(gin, b_ss).wait_send()

    out.wait()


def finish(acts, grads, dw, top, hist_a, hist_w, hist_g,
           out_acts, out_grads, out_w, out_ha, out_hw, out_hg, held_a, held_g, held_w, in_sem, out_sem):
    half = dw.shape[0] // 2
    moves = [(acts, held_a, out_acts.at[0]), (grads, held_g, out_grads.at[0])]
    for i in range(2):
        rows = pl.ds(i * half, half)
        moves.append((dw.at[rows], held_w.at[rows], out_w.at[0, rows]))
    inward = [pltpu.make_async_copy(src, held, in_sem.at[0, i]) for i, (src, held, _) in enumerate(moves)]
    outward = [pltpu.make_async_copy(held, dst, out_sem.at[0, i]) for i, (_, held, dst) in enumerate(moves)]
    for copy in inward:
        copy.start()
    peaks = top[...]
    for row, (hist, out_hist) in enumerate(((hist_a, out_ha), (hist_w, out_hw), (hist_g, out_hg))):
        old = hist[...]
        out_hist[...] = jnp.concatenate([peaks[row:row + 1, 0:1], old[:, :-1]], axis=1)
    for copy, onward in zip(inward, outward):
        copy.wait()
        onward.start()
    for onward in outward:
        onward.wait()


def shards(acts_in, weights, cotangent, hist_act, hist_weight, hist_grad):
    S, N, T = lax.axis_size("pipe"), lax.axis_size("dp"), lax.axis_size("tensor")
    M, R, F = acts_in.shape
    NC, RC = M * PIECES, R // PIECES
    FA = T * F // N
    bf, f32 = jnp.bfloat16, jnp.float32
    dma = pltpu.SemaphoreType.DMA
    vmem = pl.BlockSpec(memory_space=pltpu.VMEM)
    anyw = pl.BlockSpec(memory_space=pl.ANY)
    hist = jax.ShapeDtypeStruct(hist_act.shape, f32)
    chunk = (NC, RC, F)
    acts, grads, dw, top = pl.pallas_call(
        functools.partial(kernel, S, N, T, NC, RC, F, FA),
        out_shape=(jax.ShapeDtypeStruct(chunk, bf), jax.ShapeDtypeStruct(chunk, bf),
                   jax.ShapeDtypeStruct((FA, F), bf), jax.ShapeDtypeStruct((8, 128), f32)),
        in_specs=[vmem, anyw, vmem, vmem, vmem, vmem],
        out_specs=(anyw, anyw, anyw, vmem),
        scratch_shapes=[
            pltpu.VMEM((T, F, F), bf),
            pltpu.VMEM((T, F, F), bf),
            pltpu.VMEM((NC, T, RC, F), bf),
            pltpu.VMEM((NC, T, RC, F), bf),
            pltpu.VMEM(chunk, bf),
            pltpu.VMEM((PAIR * RC, F), f32),
            pltpu.VMEM((NC, T, RC, F), bf),
            pltpu.VMEM((2, NC, T, RC, F), bf),
            pltpu.VMEM(chunk, bf),
            pltpu.VMEM(chunk, bf),
            pltpu.VMEM((NC, N, RC, F), bf),
            pltpu.VMEM((NC, N, RC, FA), bf),
            pltpu.VMEM((FA, F), f32),
            pltpu.VMEM((FA, F), bf),
            pltpu.VMEM((N, 8, 128), f32),
            pltpu.VMEM((T, 8, 128), f32),
            pltpu.VMEM((16, F), bf),
            pltpu.VMEM((16, F), bf),
            dma((T,)), dma(()), dma(()), dma((NC, 2)), dma(()), dma(()), dma(()), dma(()),
            dma(()), dma((2, NC)), dma(()), dma((NC, N // 2)), dma(()), dma(()),
            dma(()), dma(()), dma(()), dma(()), dma((2,)), dma(()),
        ],
        compiler_params=pltpu.CompilerParams(
            collective_id=0, has_side_effects=True, vmem_limit_bytes=60 * 2**20),
    )(acts_in.reshape(chunk), weights.reshape(T, F, F), cotangent.reshape(chunk),
      hist_act, hist_weight, hist_grad)
    full = (1, M, R, F)
    return pl.pallas_call(
        finish,
        out_shape=(jax.ShapeDtypeStruct(full, bf), jax.ShapeDtypeStruct(full, bf),
                   jax.ShapeDtypeStruct((1, FA, F), bf), hist, hist, hist),
        in_specs=[anyw, anyw, anyw, vmem, vmem, vmem, vmem],
        out_specs=(anyw, anyw, anyw, vmem, vmem, vmem),
        scratch_shapes=[pltpu.VMEM((M, R, F), bf), pltpu.VMEM((M, R, F), bf),
                        pltpu.VMEM((FA, F), bf), dma((2, 4)), dma((2, 4))],
        compiler_params=pltpu.CompilerParams(vmem_limit_bytes=60 * 2**20),
    )(acts.reshape(M, R, F), grads.reshape(M, R, F), dw, top, hist_act, hist_weight, hist_grad)


def solution(mesh):
    placed = (P(None, "dp", "tensor"), P("pipe", None, "tensor"), P(None, "dp", "tensor"),
              P("pipe", None), P("pipe", None), P("pipe", None))
    return jax.shard_map(
        shards, mesh=mesh, in_specs=placed,
        out_specs=(P("pipe", None, "dp", "tensor"), P("pipe", None, "dp", "tensor"),
                   P("pipe", "dp", "tensor"), P("pipe", None), P("pipe", None), P("pipe", None)),
        check_vma=False)
```

```python
import functools

import jax
import jax.numpy as jnp
from jax import lax
from jax.experimental import pallas as pl
from jax.experimental.pallas import tpu as pltpu
from jax.sharding import PartitionSpec as P

MESH = pl.DeviceIdType.MESH
PIECES = 8
AHEAD = 6
LAG_LOW, LAG_HIGH = 2, 3
CUTS = 4
WARM = 4
UPDATES = ((0, 8), (8, 4), (12, 4))
PAIR = 2
HALVES = 2


def kernel(S, N, T, NC, RC, F, FA,
           acts_in, weights, cot_in, hists_a, hists_w, hists_g,
           out_acts, out_grads, out_w, out_top,
           acts, cot, hist_a, hist_w, hist_g, w, wt, x, xq, xo, acc, pt, pr, gin, gout, G, A, dw, dwb, pz, py, amax, gmax,
           in_sem, w_sem, i_ss, x_ss, x_rs, A_ss, A_rs, B_ss, B_rs, p_ss, p_rs, f_rs,
           G_ss, G_rs, b_ss, b_rs, z_ss, z_rs, y_ss, y_rs, o_sem, ow_sem):
    s, d, t = lax.axis_index("pipe"), lax.axis_index("dp"), lax.axis_index("tensor")
    last = S - 1
    bf, f32 = jnp.bfloat16, jnp.float32
    upper = s >= S // 2
    wide = s >= last - 1
    lag = jnp.where(s < 2, LAG_LOW, LAG_HIGH)
    tail = lag * (N // 2)
    up = jnp.minimum(s + 1, last)
    down = jnp.maximum(s - 1, 0)
    ratio = N // T
    far_hops = N // 2
    near_hops = N - 1 - far_hops
    offsets = [T // 2] + [o for o in range(1, T) if o != T // 2]

    def remote(src, dst, ss, rsem, **where):
        return pltpu.make_async_remote_copy(
            src_ref=src, dst_ref=dst, send_sem=ss, recv_sem=rsem,
            device_id=where, device_id_type=MESH)

    def peer(o):
        return lax.rem(t + o, T)

    def row(k):
        return lax.rem(d + k, N)

    barrier = pltpu.get_barrier_semaphore()
    for k in range(1, N):
        pl.semaphore_signal(barrier, inc=1, device_id={"dp": row(k)}, device_id_type=MESH)
    for o in range(1, T):
        pl.semaphore_signal(barrier, inc=1, device_id={"tensor": peer(o)}, device_id_type=MESH)

    @pl.when(s > 0)
    def _():
        for j in range(T):
            pl.semaphore_signal(barrier, inc=1, device_id={"pipe": s - 1, "tensor": j}, device_id_type=MESH)

    @pl.when(s < last)
    def _():
        for j in range(T):
            pl.semaphore_signal(barrier, inc=1, device_id={"pipe": s + 1, "tensor": j}, device_id_type=MESH)

    fills = [pltpu.make_async_copy(src, dst, in_sem.at[i]) for i, (src, dst) in enumerate((
        (hists_a, hist_a), (hists_w, hist_w), (hists_g, hist_g), (acts_in, acts), (cot_in, cot)))]
    for copy in fills:
        copy.start()
    loads = [pltpu.make_async_copy(weights.at[b], w.at[b], w_sem.at[b]) for b in range(T)]
    for copy in loads:
        copy.start()

    amax[...] = jnp.zeros_like(amax)
    gmax[...] = jnp.zeros_like(gmax)
    for copy in fills:
        copy.wait()

    lim_a = jnp.max(hist_a[...], axis=1, keepdims=True).astype(bf)
    lim_w = jnp.max(hist_w[...], axis=1, keepdims=True).astype(bf)
    lim_g = jnp.max(hist_g[...], axis=1, keepdims=True).astype(bf)

    def clip(v, lim):
        return jnp.minimum(jnp.maximum(v, -lim), lim)

    def fold(v):
        return jnp.max(jnp.abs(v).reshape(-1, 16, v.shape[-1]), axis=0)

    near = (s > 0).astype(jnp.int32) + (s < last).astype(jnp.int32)
    pl.semaphore_wait(barrier, N - 1 + T - 1 + T * near)

    def settled(ref, sem):
        return remote(ref, ref, sem, sem, tensor=peer(1))

    crossing = jnp.logical_and(s > 0, lax.rem(s, 2) == 0)
    crossing_up = lax.rem(s, 2) == 1

    def first_copy(c, o):
        return remote(acts.at[c], x.at[c, t], i_ss, x_rs.at[c, 1], tensor=peer(o))

    def x_copy(c, o, cols):
        lead = jnp.where(crossing_up, T // 2, 0) == o
        return remote(xo.at[c, :, cols], x.at[c, t, :, cols], x_ss,
                      x_rs.at[c, jnp.where(lead, 0, 1)], pipe=up, tensor=peer(o))

    def block_of(e):
        start = lax.rem(e, ratio) * FA
        return lax.div(e, ratio), pl.ds(pl.multiple_of(start, FA), FA)

    def A_copy(c, k):
        e = row(k)
        b, cols = block_of(e)
        return remote(xq.at[c, b, :, cols], A.at[c, d], A_ss, A_rs, dp=e)

    def B_copy(c, o):
        return remote(A.at[c], A.at[c], B_ss, B_rs, tensor=peer(o))

    def p_copy(c, j):
        return remote(pt.at[c, j], pr.at[0, c, t], p_ss, p_rs.at[c], pipe=down, tensor=j)

    def f_copy(c, o):
        return remote(pt.at[c, peer(o)], pr.at[1, c, t], p_ss, f_rs, tensor=peer(o))

    def back_copy(c):
        return remote(gin.at[c], out_grads.at[c], b_ss, b_rs, pipe=up)

    def turn(c):
        return jnp.where(lax.rem(c, 2) == 0, 1, N - 1)

    def G_copy(c, way, h):
        ahead = turn(c) if way == 0 else N - turn(c)
        r = row((h - 1) * (N - ahead))
        return remote(G.at[c, r], G.at[c, r], G_ss, G_rs.at[c, h - 1], dp=row(ahead))

    def z_copy(k):
        return remote(pz.at[0], pz.at[k], z_ss, z_rs, dp=row(k))

    def y_copy(o):
        return remote(py.at[0], py.at[o], y_ss, y_rs, tensor=peer(o))

    def acts_out(c):
        return pltpu.make_async_copy(xo.at[c], out_acts.at[c], o_sem.at[0])

    grads_out = pltpu.make_async_copy(gout, out_grads, o_sem.at[1])

    def each_chunk(body):
        def step(c, _):
            body(c)
            return 0

        lax.fori_loop(0, NC, step, 0)

    def send_first(c):
        for o in offsets:
            first_copy(c, o).start()

    @pl.when(s == 0)
    def _():
        for c in range(AHEAD):
            send_first(c)

        def body(c):
            x[c, t] = acts[c]

        each_chunk(body)

    peak = jnp.zeros((16, F), bf)
    for b in range(T):
        loads[b].wait()

        def squeeze(i, m, b=b):
            rows = pl.ds(pl.multiple_of(i * 128, 128), 128)
            v = w[b, rows]
            w[b, rows] = clip(v, lim_w)
            return jnp.maximum(m, fold(v))

        peak = lax.fori_loop(0, F // 128, squeeze, peak)
    top_w = jnp.max(peak.astype(f32), keepdims=True).reshape(1, 1)
    pz[0] = jnp.broadcast_to(top_w, (8, 128))

    def flip_weights():
        def turn_block(i, _):
            b, n = lax.div(i, F // 128), lax.rem(i, F // 128)
            rows = pl.ds(pl.multiple_of(n * 128, 128), 128)
            wt[b, :, rows] = w[b, rows, :].T
            return 0

        lax.fori_loop(0, T * (F // 128), turn_block, 0)

    pl.when(upper)(flip_weights)

    middle = [o for o in range(1, T) if o != T // 2]

    def forward(c, n):
        first = peer(jnp.where(crossing, T // 2, 0))
        rest = [peer(o) for o in middle] + [peer(jnp.where(crossing, 0, T // 2))]
        span, high = pl.ds(c, n), n * RC

        @pl.when(s > 0)
        def _():
            for m in range(n):
                settled(x.at[c + m, 0], x_rs.at[c + m, 0]).wait_recv()

        q = clip(x[span, first], lim_a)
        xq[span, first] = q
        acc[pl.ds(0, high)] = jnp.dot(q.reshape(high, F), w[first], preferred_element_type=f32)
        for m in range(n):
            settled(x.at[c + m, pl.ds(0, T - 1)], x_rs.at[c + m, 1]).wait_recv()
        for j in rest:
            xq[span, j] = clip(x[span, j], lim_a)
        width = F // HALVES
        for k in range(HALVES):
            cols = pl.ds(k * width, width)
            y = acc[pl.ds(0, high), cols] + x[span, t, :, cols].reshape(high, width).astype(f32)
            for j in rest:
                y = y + jnp.dot(xq[span, j].reshape(high, F), w[j, :, cols], preferred_element_type=f32)
            xo[span, :, cols] = y.astype(bf).reshape(n, RC, width)

            @pl.when(s < last)
            def _():
                for m in range(n):
                    for o in offsets + [0]:
                        x_copy(c + m, o, cols).start()

        if n == 1:
            @pl.when(jnp.logical_and(s == 0, c + AHEAD < NC))
            def _():
                send_first(jnp.minimum(c + AHEAD, NC - 1))

        for m in range(n):
            acts_out(c + m).start()

            @pl.when(lax.rem(c + m, T) == t)
            def _():
                send_A(c + m)
                b, cols = block_of(d)
                A[c + m, d] = xq[c + m, b, :, cols]

        amax[...] = jnp.maximum(amax[...], fold(x[span, t]))

    def send_A(c):
        for k in range(1, N):
            A_copy(c, k).start()

    def backward(c, n):
        span, high = pl.ds(c, n), n * RC

        def last_grads():
            gin[span] = (cot[span].astype(f32) * xo[span].astype(f32)).astype(bf)

        def summed_grads():
            for m in range(n):
                settled(pr.at[0, c + m], p_rs.at[c + m]).wait_recv()
            total = pr[0, span, 0].astype(f32)
            for j in range(1, T):
                total = total + pr[0, span, j].astype(f32)
            gin[span] = total.astype(bf)
            for m in range(n):
                back_copy(c + m).start()

        if n == 1:
            summed_grads()
        else:
            pl.when(s == last)(last_grads)
            pl.when(s < last)(summed_grads)
        g = gin[span]
        q = clip(g, lim_g)
        G[span, d] = q
        for m in range(n):
            for way in range(2):
                G_copy(c + m, way, 1).start()
        q = q.reshape(high, F)
        for group in (offsets[:2], offsets[2:] + [0]):
            for o in group:
                y = jnp.dot(q, wt[peer(o)], preferred_element_type=f32)
                if o == 0:
                    y = y + g.reshape(high, F).astype(f32)
                pt[span, peer(o)] = y.astype(bf).reshape(n, RC, F)

            @pl.when(s > 0)
            def _():
                for o in group:
                    for m in range(n):
                        p_copy(c + m, peer(o)).start()

            if n == 1:
                @pl.when(s == 0)
                def _():
                    for o in group:
                        if o:
                            f_copy(c, o).start()

        gmax[...] = jnp.maximum(gmax[...], fold(g))

        @pl.when(c == NC - n)
        def _():
            line = lax.broadcasted_iota(jnp.int32, (8, 128), 0)
            top_a = jnp.max(amax[...].astype(f32), keepdims=True).reshape(1, 1)
            top_g = jnp.max(gmax[...].astype(f32), keepdims=True).reshape(1, 1)
            pz[0] = jnp.where(line == 0, top_a, jnp.where(line == 1, pz[0], top_g))
            for k in range(1, N):
                z_copy(k).start()

    def finish_grads():
        settled(pr.at[1, :, pl.ds(0, T - 1)], f_rs).wait_recv()

        def body(c):
            total = pt[c, t].astype(f32)
            for o in range(1, T):
                total = total + pr[1, c, peer(o)].astype(f32)
            gout[c] = total.astype(bf)

        each_chunk(body)
        grads_out.start()

    def spread():
        settled(A.at[pl.ds(0, NC // T), pl.ds(0, N - 1)], A_rs).wait_recv()
        for m in range(NC // T):
            for o in offsets:
                B_copy(t + T * m, o).start()

    def relay(c, h):
        @pl.when(jnp.logical_and(c >= 0, c < NC))
        def _():
            ways = 2 if h <= near_hops else 1
            settled(G.at[c, pl.ds(0, ways)], G_rs.at[c, h - 1]).wait_recv()
            for way, hops in ((0, far_hops), (1, near_hops)):
                if h < hops:
                    G_copy(c, way, h + 1).start()

    def update(first, count):
        if first == 0:
            settled(A.at[pl.ds(0, NC - NC // T)], B_rs).wait_recv()
        tile, depth = 256, count * N * RC
        span = pl.ds(first, count)

        def body(n, _):
            cols = pl.ds(pl.multiple_of(n * tile, tile), tile)
            y = lax.dot_general(A[span, :, :, cols].reshape(depth, tile), G[span].reshape(depth, F),
                                (((0,), (0,)), ((), ())), preferred_element_type=f32)
            if first:
                y = dw[cols, :] + y
            if first + count < NC:
                dw[cols, :] = y
            else:
                dwb[cols, :] = y.astype(bf)
                pltpu.make_async_copy(dwb.at[cols], out_w.at[cols], ow_sem).start()
            return 0

        lax.fori_loop(0, FA // tile, body, 0)

    def after(c):
        for h in range(1, far_hops + 1):
            relay(c - lag * h, h)

        @pl.when(jnp.logical_and(s == 0, c == NC + 2))
        def _():
            finish_grads()

        @pl.when(jnp.logical_and(upper, c == jnp.where(wide, 4, NC)))
        def _():
            spread()

        @pl.when(c == NC + 1)
        def _():
            settled(pz.at[pl.ds(1, N - 1)], z_rs).wait_recv()
            py[0] = jnp.max(pz[...], axis=0)
            for o in range(1, T):
                y_copy(o).start()

        for first, count in UPDATES:
            @pl.when(c == first + count - 1 + tail)
            def _():
                update(first, count)

    count = jnp.where(wide, NC // PAIR, NC)
    warm = jnp.where(s == last, 1, jnp.where(wide, WARM, count))

    def slot(i, _):
        m = i - count
        turned = i - warm
        mixed = jnp.logical_and(turned >= 0, i < 2 * count - warm)
        odd = lax.rem(i + 2 * NC - warm, 2) == 1
        ahead = jnp.logical_or(turned < 0, jnp.logical_and(mixed, odd))
        turn_c = jnp.where(turned < 0, i, jnp.where(mixed, lax.div(turned, 2) + jnp.where(odd, warm, 0), m))
        paired = m < 2 * NC
        even = lax.rem(i + NC, 2) == 0
        is_fwd = jnp.where(wide, jnp.logical_and(ahead, i < 2 * count), i < NC)
        is_bwd = jnp.where(wide, jnp.logical_and(jnp.logical_not(ahead), i < 2 * count),
                           jnp.logical_and(jnp.logical_and(m >= 0, paired), even))
        c_after = jnp.where(wide, i - 2 * count, jnp.where(paired, lax.div(m, 2), m - NC))
        is_after = jnp.logical_and(jnp.logical_not(jnp.logical_or(is_fwd, is_bwd)), c_after < NC + tail)
        c_fwd = jnp.where(wide, turn_c, i)
        c_bwd = jnp.where(wide, turn_c, lax.div(m, 2))

        @pl.when(jnp.logical_and(i == NC, jnp.logical_not(upper)))
        def _():
            flip_weights()
            spread()

        for body, on, c in ((forward, is_fwd, c_fwd), (backward, is_bwd, c_bwd)):
            @pl.when(jnp.logical_and(on, jnp.logical_not(wide)))
            def _():
                body(c, 1)

            @pl.when(jnp.logical_and(on, wide))
            def _():
                body(PAIR * c, PAIR)

        @pl.when(is_after)
        def _():
            after(c_after)

        return 0

    lax.fori_loop(0, 3 * NC + far_hops * max(LAG_LOW, LAG_HIGH), slot, 0)

    settled(py.at[pl.ds(1, T - 1)], y_rs).wait_recv()
    out_top[...] = jnp.max(py[...], axis=0)

    settled(A.at[pl.ds(0, NC // T), pl.ds(0, N - 1)], A_ss).wait_send()
    settled(A.at[pl.ds(0, NC - NC // T)], B_ss).wait_send()
    settled(G.at[:, pl.ds(0, N - 1)], G_ss).wait_send()
    settled(pz.at[pl.ds(1, N - 1)], z_ss).wait_send()
    settled(py.at[pl.ds(1, T - 1)], y_ss).wait_send()
    pltpu.make_async_copy(xo, out_acts, o_sem.at[0]).wait()

    @pl.when(s == 0)
    def _():
        settled(x.at[:, pl.ds(0, T - 1)], i_ss).wait_send()
        settled(pt.at[:, pl.ds(0, T - 1)], p_ss).wait_send()
        grads_out.wait()

    @pl.when(s > 0)
    def _():
        settled(pt, p_ss).wait_send()
        settled(out_grads, b_rs).wait_recv()

    @pl.when(s < last)
    def _():
        settled(x, x_ss).wait_send()
        settled(gin, b_ss).wait_send()

    pltpu.make_async_copy(dwb, out_w, ow_sem).wait()


def finish(acts, grads, dw, top, hist_a, hist_w, hist_g,
           out_acts, out_grads, out_w, out_ha, out_hw, out_hg, held_a, held_g, held_w, in_sem, out_sem):
    moves = [(acts, held_a, out_acts.at[0]), (grads, held_g, out_grads.at[0])]
    part = dw.shape[0] // CUTS
    for i in range(CUTS):
        rows = pl.ds(i * part, part)
        moves.append((dw.at[rows], held_w.at[rows], out_w.at[0, rows]))
    inward = [pltpu.make_async_copy(src, held, in_sem.at[i]) for i, (src, held, _) in enumerate(moves)]
    outward = [pltpu.make_async_copy(held, dst, out_sem.at[i]) for i, (_, held, dst) in enumerate(moves)]
    for copy in inward:
        copy.start()
    peaks = top[...]
    for row, (hist, out_hist) in enumerate(((hist_a, out_ha), (hist_w, out_hw), (hist_g, out_hg))):
        old = hist[...]
        out_hist[...] = jnp.concatenate([peaks[row:row + 1, 0:1], old[:, :-1]], axis=1)
    for copy, onward in zip(inward, outward):
        copy.wait()
        onward.start()
    for onward in outward:
        onward.wait()


def shards(acts_in, weights, cotangent, hist_act, hist_weight, hist_grad):
    S, N, T = lax.axis_size("pipe"), lax.axis_size("dp"), lax.axis_size("tensor")
    M, R, F = acts_in.shape
    NC, RC = M * PIECES, R // PIECES
    FA = T * F // N
    bf, f32 = jnp.bfloat16, jnp.float32
    dma = pltpu.SemaphoreType.DMA
    vmem = pl.BlockSpec(memory_space=pltpu.VMEM)
    anyw = pl.BlockSpec(memory_space=pl.ANY)
    hbm = pl.BlockSpec(memory_space=pltpu.HBM)
    hist = jax.ShapeDtypeStruct(hist_act.shape, f32)
    chunk = (NC, RC, F)
    acts, grads, dw, top = pl.pallas_call(
        functools.partial(kernel, S, N, T, NC, RC, F, FA),
        out_shape=(jax.ShapeDtypeStruct(chunk, bf), jax.ShapeDtypeStruct(chunk, bf),
                   jax.ShapeDtypeStruct((FA, F), bf), jax.ShapeDtypeStruct((8, 128), f32)),
        in_specs=[hbm] * 6,
        out_specs=(anyw, anyw, anyw, vmem),
        scratch_shapes=[
            pltpu.VMEM(chunk, bf),
            pltpu.VMEM(chunk, bf),
            pltpu.VMEM(hist_act.shape, f32),
            pltpu.VMEM(hist_act.shape, f32),
            pltpu.VMEM(hist_act.shape, f32),
            pltpu.VMEM((T, F, F), bf),
            pltpu.VMEM((T, F, F), bf),
            pltpu.VMEM((NC, T, RC, F), bf),
            pltpu.VMEM((NC, T, RC, F), bf),
            pltpu.VMEM(chunk, bf),
            pltpu.VMEM((PAIR * RC, F), f32),
            pltpu.VMEM((NC, T, RC, F), bf),
            pltpu.VMEM((2, NC, T, RC, F), bf),
            pltpu.VMEM(chunk, bf),
            pltpu.VMEM(chunk, bf),
            pltpu.VMEM((NC, N, RC, F), bf),
            pltpu.VMEM((NC, N, RC, FA), bf),
            pltpu.VMEM((FA, F), f32),
            pltpu.VMEM((FA, F), bf),
            pltpu.VMEM((N, 8, 128), f32),
            pltpu.VMEM((T, 8, 128), f32),
            pltpu.VMEM((16, F), bf),
            pltpu.VMEM((16, F), bf),
            dma((5,)), dma((T,)), dma(()), dma(()), dma((NC, 2)), dma(()), dma(()), dma(()), dma(()),
            dma(()), dma((NC,)), dma(()), dma(()), dma((NC, N // 2)), dma(()), dma(()),
            dma(()), dma(()), dma(()), dma(()), dma((2,)), dma(()),
        ],
        compiler_params=pltpu.CompilerParams(
            collective_id=0, has_side_effects=True, vmem_limit_bytes=60 * 2**20),
    )(acts_in.reshape(chunk), weights.reshape(T, F, F), cotangent.reshape(chunk),
      hist_act, hist_weight, hist_grad)
    full = (1, M, R, F)
    return pl.pallas_call(
        finish,
        out_shape=(jax.ShapeDtypeStruct(full, bf), jax.ShapeDtypeStruct(full, bf),
                   jax.ShapeDtypeStruct((1, FA, F), bf), hist, hist, hist),
        in_specs=[anyw, anyw, anyw, vmem, vmem, vmem, vmem],
        out_specs=(anyw, anyw, anyw, vmem, vmem, vmem),
        scratch_shapes=[pltpu.VMEM((M, R, F), bf), pltpu.VMEM((M, R, F), bf),
                        pltpu.VMEM((FA, F), bf), dma((2 + CUTS,)), dma((2 + CUTS,))],
        compiler_params=pltpu.CompilerParams(vmem_limit_bytes=60 * 2**20),
    )(acts.reshape(M, R, F), grads.reshape(M, R, F), dw, top, hist_act, hist_weight, hist_grad)


def solution(mesh):
    placed = (P(None, "dp", "tensor"), P("pipe", None, "tensor"), P(None, "dp", "tensor"),
              P("pipe", None), P("pipe", None), P("pipe", None))
    return jax.shard_map(
        shards, mesh=mesh, in_specs=placed,
        out_specs=(P("pipe", None, "dp", "tensor"), P("pipe", None, "dp", "tensor"),
                   P("pipe", "dp", "tensor"), P("pipe", None), P("pipe", None), P("pipe", None)),
        check_vma=False)
```
